128 devices in a mesh: seq: 32 (over x, z, y_lo), doc: 4 (over y_hi, core).
Axes of the slice: x: 4, y: 4 (y_hi: 2, y_lo: 2; y = y_hi * 2 + y_lo), z: 4, core: 2. Of those that a mesh axis runs over, the one named last changes fastest.
Arguments:
- queries: bfloat16 [65536, 4096], P(('doc', 'seq')), parts along dimension 0, may hold values from -24 to 24
- keys: bfloat16 [65536, 4096], P(('doc', 'seq')), parts along dimension 0, may hold values from -24 to 24
- values: bfloat16 [65536, 4096], P(('doc', 'seq')), parts along dimension 0, may hold values from -6 to 6
Outputs:
- attended: bfloat16 [65536, 4096], P(('doc', 'seq')), parts along dimension 0
The draws below stay inside these ranges and needn't reach their ends.
There are 4 independent parts, one for each index of `doc`. The reference program is written for one: setup_inputs(seed, part) draws one part's arguments, and reference() takes and returns one part's arrays. A program takes and returns all parts, laid end to end along the dimension named above; each array names one. Nothing has to cross between parts.
All inputs are finite; a program needn't handle non-finite values. Where the reference program divides by a largest or mean magnitude, that divisor is 1e-20 or more.
Results may differ from the reference program's by a relative error of at most 0.04.
Values may be sent and summed in bfloat16 or wider, within the bound.
No kernel may reach another device: no remote copies, remote signals or barrier semaphores. Data moves between devices by JAX's collectives and lax.ppermute only.
A program may use at most 192 MiB of HBM per device.

```python
import jax
import jax.numpy as jnp
from jax import lax

H = 32
DH = 128
M = 512
ITERS = 6
D = 4096
TOKENS = 16384


def structured_field(key, salt):
    segment = TOKENS // M
    means = 1.2 * jax.random.truncated_normal(jax.random.fold_in(key, salt), -4.0, 4.0, (M, D), jnp.float32)
    noise = 0.8 * jax.random.truncated_normal(jax.random.fold_in(key, salt + 40), -4.0, 4.0, (TOKENS, D), jnp.float32)
    return (jnp.repeat(means, segment, axis=0) + noise).astype(jnp.bfloat16)


def draw_queries(key, part):
    return structured_field(key, 1)


def draw_keys(key, part):
    return structured_field(key, 2)


def block_levels(own_key, shape, split, least, largest):
    gain = 1.0
    for axis_at, parts in split:
        heights = jax.random.uniform(jax.random.fold_in(jax.random.fold_in(own_key, 6), axis_at), (parts,), jnp.float32, least / len(split), largest / len(split))
        gain = gain * jnp.repeat(jnp.exp(heights), shape[axis_at] // parts).reshape((-1,) + (1,) * (len(shape) - 1 - axis_at))
    return gain


def centred(rng, dims, width, reach, pieces=(), kind=jnp.bfloat16):
    array = width * jax.random.normal(rng, dims, jnp.float32)
    if pieces:
        array = array * block_levels(rng, dims, pieces, -0.22, 0.18)
    return jnp.clip(array, -reach, reach).astype(kind)


def setup_inputs(seed: int = 0, part: int = 0) -> dict:
    seeds = jax.random.split(jax.random.key(seed), 4)
    part_keys = jax.random.split(jax.random.fold_in(seeds[3], part), 4)
    queries = draw_queries(jax.random.fold_in(jax.random.fold_in(seeds[3], part), 71), part)
    keys = draw_keys(jax.random.fold_in(jax.random.fold_in(seeds[3], part), 71), part)
    values = centred(part_keys[2], (TOKENS, D), 1.0, 6.0, ((0, 32),))
    return {"queries": queries, "keys": keys, "values": values}


def softmax_last(scores):
    top = jnp.max(scores, -1, keepdims=True)
    exponent_values = jnp.exp(scores - top)
    return exponent_values / jnp.sum(exponent_values, -1, keepdims=True)


def newton_schulz(kernel):
    precise = lax.Precision.HIGHEST
    row_most = jnp.max(jnp.sum(jnp.abs(kernel), 1))
    col_most = jnp.max(jnp.sum(jnp.abs(kernel), 0))
    inverse = kernel.T / (row_most * col_most)
    identity = jnp.eye(kernel.shape[0], dtype=jnp.float32)
    for sweep in range(ITERS):
        kernel_inv = jnp.dot(kernel, inverse, precision=precise)
        inner = jnp.dot(kernel_inv, 7.0 * identity - kernel_inv, precision=precise)
        middle = jnp.dot(kernel_inv, 15.0 * identity - inner, precision=precise)
        inverse = 0.25 * jnp.dot(inverse, 13.0 * identity - middle, precision=precise)
    return inverse


def reference(queries, keys, values):
    segment = TOKENS // M
    score_scale = DH ** -0.5
    land_q = (jnp.sum(queries.reshape(M, segment, D).astype(jnp.float32), 1) / segment).astype(jnp.bfloat16)
    land_k = (jnp.sum(keys.reshape(M, segment, D).astype(jnp.float32), 1) / segment).astype(jnp.bfloat16)

    def per_head(head):
        offset = (head * DH).astype(jnp.int32)
        head_q = lax.dynamic_slice_in_dim(queries, offset, DH, 1)
        head_k = lax.dynamic_slice_in_dim(keys, offset, DH, 1)
        head_v = lax.dynamic_slice_in_dim(values, offset, DH, 1)
        query_landmark_means = lax.dynamic_slice_in_dim(land_q, offset, DH, 1)
        key_landmark_means = lax.dynamic_slice_in_dim(land_k, offset, DH, 1)
        kernel = softmax_last(jnp.dot(query_landmark_means, key_landmark_means.T, preferred_element_type=jnp.float32) * score_scale)
        inverse = newton_schulz(kernel).astype(jnp.bfloat16)
        scores_b = jnp.dot(query_landmark_means, head_k.T, preferred_element_type=jnp.float32) * score_scale
        peak = jnp.max(scores_b, 1, keepdims=True)
        exponent_values = jnp.exp(scores_b - peak)
        totals = jnp.sum(exponent_values, 1, keepdims=True)
        weighted = jnp.dot(exponent_values.astype(jnp.bfloat16), head_v, preferred_element_type=jnp.float32)
        normalized_rows = (weighted / totals).astype(jnp.bfloat16)
        attention_product = jnp.dot(inverse, normalized_rows, preferred_element_type=jnp.float32).astype(jnp.bfloat16)
        attention_weight = softmax_last(jnp.dot(head_q, key_landmark_means.T, preferred_element_type=jnp.float32) * score_scale).astype(jnp.bfloat16)
        return jnp.dot(attention_weight, attention_product, preferred_element_type=jnp.float32).astype(jnp.bfloat16)

    results = lax.map(per_head, jnp.arange(H, dtype=jnp.int32))
    return jnp.transpose(results, (1, 0, 2)).reshape(TOKENS, D)
```

```python
import math

import jax
import jax.numpy as jnp
from jax import lax
from jax.experimental import pallas as pl
from jax.experimental.pallas import tpu as pltpu
from jax.sharding import Mesh
from jax.sharding import PartitionSpec as P


H = 32
DH = 128
M = 512
ITERS = 6
D = 4096
SEQ = ("x", "z", "y")
DOC_SEQ = ("doc", "x", "z", "y")
C2 = DH ** (-0.5) * math.log2(math.e)
F32 = jnp.float32
BF16 = jnp.bfloat16
EXTRA = 16
ROWS = M // 32
GROUP = 4
LAST = 8
TALL = 128


def shifted(v, axis, by):
    n = lax.axis_size(axis)
    return lax.ppermute(v, axis, [(i, (i + by) % n) for i in range(n)])


def ring(v, axis):
    return [v] + [shifted(v, axis, s) for s in (1, 3, 2)]


def in_slots(parts):
    own, one, three, two = parts
    return [own, one, two, three]


def gather_first(v):
    both = jnp.stack([v, shifted(v, "y", 1)])
    half = both.shape[-1] // 2
    return (in_slots(ring(both[..., :half], "x")), in_slots(ring(both[..., half:], "z")))


def place(pos, slot_x, slot_z, slot_y):
    jx = (pos[0] + 4 - slot_x) % 4
    jz = (pos[1] + 4 - slot_z) % 4
    jy = (pos[2] + slot_y) % 2
    return (jx * 4 + jz) * 2 + jy


def fill_table(pos, table):
    for later in range(4):
        for early in range(4):
            for slot_y in range(2):
                at = (later * 4 + early) * 2 + slot_y
                table[at] = place(pos, early, later, slot_y) * ROWS
                table[32 + at] = place(pos, later, early, slot_y) * ROWS


def spread(table, base, pieces, out):
    for later, piece in enumerate(pieces):
        for early in range(4):
            for slot_y in range(2):
                at = pl.multiple_of(table[base + (later * 4 + early) * 2 + slot_y], ROWS)
                out[pl.ds(at, ROWS), :] = piece[early, slot_y]


def spread_head(table, head, pieces_a, pieces_b, out):
    @pl.when(head < H // 2)
    def _():
        spread(table, 0, pieces_a, out)

    @pl.when(head >= H // 2)
    def _():
        spread(table, 32, pieces_b, out)


def piece_specs(block_of, heads):
    shape = (4, 2, ROWS, heads * DH)
    last = H // 2 // heads
    a = pl.BlockSpec(shape, lambda *g: (0, 0, 0, jnp.minimum(block_of(*g), last - 1)))
    b = pl.BlockSpec(shape, lambda *g: (0, 0, 0, jnp.maximum(block_of(*g) - last, 0)))
    return [a] * 4 + [b] * 4


def nt(a, b):
    return lax.dot_general(a, b, (((1,), (1,)), ((), ())), preferred_element_type=F32)


def parts_kernel(pos, keys, values, *rest):
    pieces, (out, land, table) = rest[:8], rest[8:]
    g = pl.program_id(0)

    @pl.when(g == 0)
    def _():
        fill_table(pos, table)

    spread_head(table, g * GROUP, pieces[:4], pieces[4:], land)

    def scores_of(j):
        return nt(keys[:, j * DH : (j + 1) * DH], land[:, j * DH : (j + 1) * DH])

    def expo_of(scores):
        top = jnp.max(scores, 0, keepdims=True)
        expo = jnp.exp2(scores * C2 - top * C2)
        return top, expo.astype(BF16), jnp.sum(expo, 0, keepdims=True)

    def store(j, top, expo, totals):
        weighted = lax.dot_general(
            values[:, j * DH : (j + 1) * DH],
            expo,
            (((0,), (0,)), ((), ())),
            preferred_element_type=F32,
        )
        part = (weighted * (1.0 / totals)).astype(BF16)
        level = top * C2 + jnp.log2(totals)
        high = level.astype(BF16).astype(F32)
        mid = (level - high).astype(BF16).astype(F32)
        low = level - high - mid
        rows = []
        for k in range(0, M, 128):
            at = slice(k, k + 128)
            out[j, at, :] = part[:, at]
            rows += [high[:, at], mid[:, at], low[:, at]]
        rows.append(jnp.zeros((EXTRA - 12, 128), F32))
        out[j, M : M + EXTRA, :] = jnp.concatenate(rows, 0).astype(BF16)

    scores = scores_of(0)
    ready = None
    for j in range(GROUP):
        following = scores_of(j + 1) if j + 1 < GROUP else None
        current = expo_of(scores)
        if ready is not None:
            store(j - 1, *ready)
        ready, scores = current, following
    store(GROUP - 1, *ready)


def near_kernel(pos, queries, *rest):
    pieces, (out, land, table) = rest[:8], rest[8:]
    g = pl.program_id(0)

    @pl.when(g == 0)
    def _():
        fill_table(pos, table)

    spread_head(table, g * GROUP, pieces[:4], pieces[4:], land)
    for j in range(GROUP):
        cols = slice(j * DH, (j + 1) * DH)
        for t in range(0, queries.shape[0], TALL):
            near = nt(queries[t : t + TALL, cols], land[:, cols])
            top = jnp.max(near, 1, keepdims=True)
            expo = jnp.exp2(near * C2 - top * C2)
            totals = jnp.sum(expo, 1, keepdims=True)
            out[j, t : t + TALL] = (expo * (1.0 / totals)).astype(BF16)


def inverse_kernel(pos, *rest):
    pieces, (out, land_q, land_k, table) = rest[:16], rest[16:]
    fill_table(pos, table)
    head = place(pos, 0, 0, 0)
    spread_head(table, head, pieces[:4], pieces[4:8], land_q)
    spread_head(table, head, pieces[8:12], pieces[12:], land_k)
    scores = nt(land_q[...], land_k[...])
    top = jnp.max(scores, 1, keepdims=True)
    expo = jnp.exp2((scores - top) * C2)
    kernel = expo / jnp.sum(expo, 1, keepdims=True)
    row_most = jnp.max(jnp.sum(jnp.abs(kernel), 1, keepdims=True))
    col_most = jnp.max(jnp.sum(jnp.abs(kernel), 0, keepdims=True))
    low = kernel.astype(BF16)
    inverse = kernel.T / (row_most * col_most)

    def dot(a, b):
        return jnp.dot(a, b, preferred_element_type=F32)

    def sweep(_, inverse):
        inv = inverse.astype(BF16)
        prod = dot(low, inv)
        p = prod.astype(BF16)
        inner = 7.0 * prod - dot(p, p)
        middle = 15.0 * prod - dot(p, inner.astype(BF16))
        return 0.25 * (13.0 * inverse - dot(inv, middle.astype(BF16)))

    out[...] = lax.fori_loop(0, ITERS, sweep, inverse).astype(BF16)


def product_kernel(parts, levels, inverse, out, acc):
    c = pl.program_id(0)
    level = jnp.zeros((32, 128), F32)
    for k in range(4):
        rows = [levels[:, 3 * k + t, :].astype(F32) for t in range(3)]
        level = jnp.where(c == k, rows[0] + rows[1] + rows[2], level)
    weight = jnp.exp2(level - jnp.max(level, 0, keepdims=True))
    weight = weight / jnp.sum(weight, 0, keepdims=True)
    normed = jnp.zeros((128, 128), F32)
    for s in range(32):
        normed = normed + parts[s].astype(F32) * weight[s : s + 1]
    part = nt(inverse[...], normed.astype(BF16))

    @pl.when(c == 0)
    def _():
        acc[...] = part

    @pl.when(c > 0)
    def _():
        acc[...] += part

    @pl.when(c == 3)
    def _():
        out[...] = acc[...].astype(BF16)


def final_kernel(pos, weights, *rest):
    pieces, (out, prod) = rest[:8], rest[8:]
    g = pl.program_id(0)
    half = M // 2

    @pl.when(g == 0)
    def _():
        for slot_x in range(4):
            for slot_z in range(4):
                for slot_y in range(2):
                    at = (slot_x * 4 + slot_z) * 2 + slot_y
                    prod[at, :half] = pieces[slot_z][slot_x, slot_y]
                    prod[at, half:] = pieces[4 + slot_x][slot_z, slot_y]

    for j in range(LAST):
        head = g * LAST + j
        jx, jz, jy = head // 8, (head // 2) % 4, head % 2
        slot_x, slot_z = (pos[0] + 4 - jx) % 4, (pos[1] + 4 - jz) % 4
        at = (slot_x * 4 + slot_z) * 2 + (pos[2] + jy) % 2
        both = jnp.dot(weights[j], prod[at], preferred_element_type=F32)
        out[:, j * DH : (j + 1) * DH] = both.astype(BF16)


def call(kernel, grid, in_specs, out_spec, out_shape, scratch, prefetch=1):
    return pl.pallas_call(
        kernel,
        grid_spec=pltpu.PrefetchScalarGridSpec(
            num_scalar_prefetch=prefetch,
            grid=grid,
            in_specs=in_specs,
            out_specs=out_spec,
            scratch_shapes=scratch,
        ),
        out_shape=out_shape,
        compiler_params=pltpu.CompilerParams(dimension_semantics=("arbitrary",) * len(grid)),
    )


def landmarks(tokens, per_device):
    segment = tokens.shape[0] // per_device
    sums = jnp.sum(tokens.reshape(per_device, segment, D), axis=1, dtype=F32)
    return (sums / segment).astype(BF16)


def steps(queries, keys, values):
    pos = jnp.stack([lax.axis_index(a) for a in SEQ]).astype(jnp.int32)
    here = queries.shape[0]
    per_device = M // 32
    means = jnp.stack([landmarks(queries, per_device), landmarks(keys, per_device)])
    first_a, first_b = gather_first(means)
    q_a = in_slots(ring(jnp.stack([p[:, 0] for p in first_a]), "z"))
    q_b = in_slots(ring(jnp.stack([p[:, 0] for p in first_b]), "x"))
    k_a = in_slots(ring(jnp.stack([p[:, 1] for p in first_a]), "z"))
    k_b = in_slots(ring(jnp.stack([p[:, 1] for p in first_b]), "x"))

    column = pl.BlockSpec((here, GROUP * DH), lambda h, pos: (0, h))
    per_head = piece_specs(lambda h, pos: h, GROUP)
    land = pltpu.VMEM((M, GROUP * DH), BF16)
    table = pltpu.SMEM((64,), jnp.int32)
    parts = call(
        parts_kernel,
        (H // GROUP,),
        [column, column] + per_head,
        pl.BlockSpec((GROUP, M + EXTRA, DH), lambda h, pos: (h, 0, 0)),
        jax.ShapeDtypeStruct((H, M + EXTRA, DH), BF16),
        [land, table],
    )(pos, keys, values, *q_a, *q_b)
    parts = lax.all_to_all(parts, SEQ, split_axis=0, concat_axis=0, tiled=True)

    weights = call(
        near_kernel,
        (H // GROUP,),
        [column] + per_head,
        pl.BlockSpec((GROUP, here, M), lambda h, pos: (h, 0, 0)),
        jax.ShapeDtypeStruct((H, here, M), BF16),
        [land, table],
    )(pos, queries, *k_a, *k_b)

    owned = piece_specs(lambda g, pos: place(pos, 0, 0, 0), 1)
    inverse = call(
        inverse_kernel,
        (1,),
        owned + owned,
        pl.BlockSpec((M, M), lambda g, pos: (0, 0)),
        jax.ShapeDtypeStruct((M, M), BF16),
        [pltpu.VMEM((M, DH), BF16)] * 2 + [table],
    )(pos, *q_a, *q_b, *k_a, *k_b)

    product = call(
        product_kernel,
        (4,),
        [
            pl.BlockSpec((H, DH, 128), lambda c: (0, c, 0)),
            pl.BlockSpec((H, EXTRA, 128), lambda c: (0, M // EXTRA, 0)),
            pl.BlockSpec((M, 128), lambda c: (0, c)),
        ],
        pl.BlockSpec((M, DH), lambda c: (0, 0)),
        jax.ShapeDtypeStruct((M, DH), BF16),
        [pltpu.VMEM((M, DH), F32)],
        prefetch=0,
    )(parts, parts, inverse)

    both = jnp.stack([product, shifted(product, "y", 1)])
    half = M // 2
    p_a = in_slots(ring(jnp.stack(in_slots(ring(both[:, :half], "x"))), "z"))
    p_b = in_slots(ring(jnp.stack(in_slots(ring(both[:, half:], "z"))), "x"))

    whole = pl.BlockSpec((4, 2, half, DH), lambda g, pos: (0, 0, 0, 0))

    return call(
        final_kernel,
        (H // LAST,),
        [pl.BlockSpec((LAST, here, M), lambda g, pos: (g, 0, 0))] + [whole] * 8,
        pl.BlockSpec((here, LAST * DH), lambda g, pos: (0, g)),
        jax.ShapeDtypeStruct((here, D), BF16),
        [pltpu.VMEM((H, M, DH), BF16)],
    )(pos, weights, *p_a, *p_b)


def solution(mesh):
    torus = Mesh(mesh.devices.reshape(4, 4, 2, mesh.shape["doc"]), ("x", "z", "y", "doc"))
    spec = P(DOC_SEQ, None)
    return jax.shard_map(
        steps, mesh=torus, in_specs=(spec, spec, spec), out_specs=spec, check_vma=False
    )
```

```python
import functools
import math

import jax
import jax.numpy as jnp
from jax import lax
from jax.experimental import pallas as pl
from jax.experimental.pallas import tpu as pltpu
from jax.sharding import Mesh
from jax.sharding import PartitionSpec as P


H = 32
DH = 128
M = 512
ITERS = 6
D = 4096
SEQ = ("x", "z", "y")
DOC_SEQ = ("doc", "x", "z", "y")
C2 = DH ** (-0.5) * math.log2(math.e)
F32 = jnp.float32
BF16 = jnp.bfloat16
EXTRA = 16
ROWS = M // 32
GROUP = 4
LAST = 8
TALL = 128


def shifted(v, axis, by):
    n = lax.axis_size(axis)
    return lax.ppermute(v, axis, [(i, (i + by) % n) for i in range(n)])


def ring(v, axis):
    return [v] + [shifted(v, axis, s) for s in (1, 3, 2)]


def in_slots(parts):
    own, one, three, two = parts
    return [own, one, two, three]


def gather_rows(v):
    both = jnp.stack([v, shifted(v, "y", 1)])
    half = both.shape[-1] // 2
    a = jnp.stack(in_slots(ring(both[..., :half], "x")))
    b = jnp.stack(in_slots(ring(both[..., half:], "z")))
    return in_slots(ring(a, "z")), in_slots(ring(b, "x"))


def place(pos, slot_x, slot_z, slot_y):
    jx = (pos[0] + 4 - slot_x) % 4
    jz = (pos[1] + 4 - slot_z) % 4
    jy = (pos[2] + slot_y) % 2
    return (jx * 4 + jz) * 2 + jy


def fill_table(pos, table):
    for later in range(4):
        for early in range(4):
            for slot_y in range(2):
                at = (later * 4 + early) * 2 + slot_y
                table[at] = place(pos, early, later, slot_y) * ROWS
                table[32 + at] = place(pos, later, early, slot_y) * ROWS


def spread(table, base, pieces, out):
    for later, piece in enumerate(pieces):
        for early in range(4):
            for slot_y in range(2):
                at = pl.multiple_of(table[base + (later * 4 + early) * 2 + slot_y], ROWS)
                out[pl.ds(at, ROWS), :] = piece[early, slot_y]


def spread_head(table, head, pieces_a, pieces_b, out):
    @pl.when(head < H // 2)
    def _():
        spread(table, 0, pieces_a, out)

    @pl.when(head >= H // 2)
    def _():
        spread(table, 32, pieces_b, out)


def piece_specs(block_of, heads):
    shape = (4, 2, ROWS, heads * DH)
    last = H // 2 // heads
    a = pl.BlockSpec(shape, lambda *g: (0, 0, 0, jnp.minimum(block_of(*g), last - 1)))
    b = pl.BlockSpec(shape, lambda *g: (0, 0, 0, jnp.maximum(block_of(*g) - last, 0)))
    return [a] * 4 + [b] * 4


def nt(a, b):
    return lax.dot_general(a, b, (((1,), (1,)), ((), ())), preferred_element_type=F32)


def parts_kernel(pos, keys, values, *rest):
    pieces, (out, land, table) = rest[:8], rest[8:]
    g = pl.program_id(0)

    @pl.when(g == 0)
    def _():
        fill_table(pos, table)

    spread_head(table, g * GROUP, pieces[:4], pieces[4:], land)

    def scores_of(j):
        return nt(keys[:, j * DH : (j + 1) * DH], land[:, j * DH : (j + 1) * DH])

    def expo_of(scores):
        top = jnp.max(scores, 0, keepdims=True)
        expo = jnp.exp2(scores * C2 - top * C2)
        return top, expo.astype(BF16), jnp.sum(expo, 0, keepdims=True)

    def store(j, top, expo, totals):
        weighted = lax.dot_general(
            values[:, j * DH : (j + 1) * DH],
            expo,
            (((0,), (0,)), ((), ())),
            preferred_element_type=F32,
        )
        part = (weighted * (1.0 / totals)).astype(BF16)
        level = top * C2 + jnp.log2(totals)
        high = level.astype(BF16).astype(F32)
        mid = (level - high).astype(BF16).astype(F32)
        low = level - high - mid
        rows = []
        for k in range(0, M, 128):
            at = slice(k, k + 128)
            out[j, at, :] = part[:, at]
            rows += [high[:, at], mid[:, at], low[:, at]]
        rows.append(jnp.zeros((EXTRA - 12, 128), F32))
        out[j, M : M + EXTRA, :] = jnp.concatenate(rows, 0).astype(BF16)

    scores = scores_of(0)
    ready = None
    for j in range(GROUP):
        following = scores_of(j + 1) if j + 1 < GROUP else None
        current = expo_of(scores)
        if ready is not None:
            store(j - 1, *ready)
        ready, scores = current, following
    store(GROUP - 1, *ready)


def near_kernel(pos, queries, *rest):
    pieces, (out, land, table) = rest[:8], rest[8:]
    g = pl.program_id(0)

    @pl.when(g == 0)
    def _():
        fill_table(pos, table)

    spread_head(table, g * GROUP, pieces[:4], pieces[4:], land)
    for j in range(GROUP):
        cols = slice(j * DH, (j + 1) * DH)
        for t in range(0, queries.shape[0], TALL):
            near = nt(queries[t : t + TALL, cols], land[:, cols])
            top = jnp.max(near, 1, keepdims=True)
            expo = jnp.exp2(near * C2 - top * C2)
            totals = jnp.sum(expo, 1, keepdims=True)
            out[j, t : t + TALL] = (expo * (1.0 / totals)).astype(BF16)


def inverse_kernel(pos, *rest):
    pieces, (out, land_q, land_k, table) = rest[:16], rest[16:]
    fill_table(pos, table)
    head = place(pos, 0, 0, 0)
    spread_head(table, head, pieces[:4], pieces[4:8], land_q)
    spread_head(table, head, pieces[8:12], pieces[12:], land_k)
    scores = nt(land_q[...], land_k[...])
    top = jnp.max(scores, 1, keepdims=True)
    expo = jnp.exp2((scores - top) * C2)
    kernel = expo / jnp.sum(expo, 1, keepdims=True)
    row_most = jnp.max(jnp.sum(jnp.abs(kernel), 1, keepdims=True))
    col_most = jnp.max(jnp.sum(jnp.abs(kernel), 0, keepdims=True))
    low = kernel.astype(BF16)
    inverse = kernel.T / (row_most * col_most)

    def dot(a, b):
        return jnp.dot(a, b, preferred_element_type=F32)

    def sweep(_, inverse):
        inv = inverse.astype(BF16)
        prod = dot(low, inv)
        p = prod.astype(BF16)
        inner = 7.0 * prod - dot(p, p)
        middle = 15.0 * prod - dot(p, inner.astype(BF16))
        return 0.25 * (13.0 * inverse - dot(inv, middle.astype(BF16)))

    out[...] = lax.fori_loop(0, ITERS, sweep, inverse).astype(BF16)


def product_kernel(parts, levels, inverse, out, acc):
    c = pl.program_id(0)
    level = jnp.zeros((32, 128), F32)
    for k in range(4):
        rows = [levels[:, 3 * k + t, :].astype(F32) for t in range(3)]
        level = jnp.where(c == k, rows[0] + rows[1] + rows[2], level)
    weight = jnp.exp2(level - jnp.max(level, 0, keepdims=True))
    weight = weight / jnp.sum(weight, 0, keepdims=True)
    normed = jnp.zeros((128, 128), F32)
    for s in range(32):
        normed = normed + parts[s].astype(F32) * weight[s : s + 1]
    part = nt(inverse[...], normed.astype(BF16))

    @pl.when(c == 0)
    def _():
        acc[...] = part

    @pl.when(c > 0)
    def _():
        acc[...] += part

    @pl.when(c == 3)
    def _():
        out[...] = acc[...].astype(BF16)


def final_kernel(shifts, pos, weights, *rest):
    n = LAST * len(shifts)
    given = rest[: 2 * len(shifts)]
    out, tiles, results, prods, sems_in, sems_out, sems_prod = rest[-7:]
    heads = []
    for shift in shifts:
        x, z = (pos[0] + 4 - shift) % 4, (pos[1] + 4 - shift) % 4
        heads += [(((pos[0] + 4 - early) % 4) * 4 + z) * 2 for early in range(4)]
        heads += [(x * 4 + (pos[1] + 4 - early) % 4) * 2 + 1 for early in range(4)]
    pieces = [
        pltpu.make_async_copy(piece, prods.at[i], sems_prod.at[i]) for i, piece in enumerate(given)
    ]
    into = [
        pltpu.make_async_copy(weights.at[h], tiles.at[i], sems_in.at[i]) for i, h in enumerate(heads)
    ]
    back = [
        pltpu.make_async_copy(
            results.at[i],
            out.at[:, pl.ds(pl.multiple_of(h * DH, DH), DH)],
            sems_out.at[i],
        )
        for i, h in enumerate(heads)
    ]
    for copy in pieces + into:
        copy.start()
    for copy in pieces:
        copy.wait()
    for first in range(0, n, 4):
        for i in range(first, first + 4):
            into[i].wait()
        held = None
        for i in range(first, first + 4):
            both = jnp.dot(tiles[i], prods[i // 4, i % 4], preferred_element_type=F32)
            if held is not None:
                results[i - 1] = held.astype(BF16)
            held = both
        results[first + 3] = held.astype(BF16)
        for i in range(first, first + 4):
            back[i].start()
    for copy in back:
        copy.wait()


def final(shifts, pos, weights, pieces, *out):
    anywhere = pl.BlockSpec(memory_space=pl.ANY)
    here = weights.shape[1]
    n = LAST * len(shifts)
    return pl.pallas_call(
        functools.partial(final_kernel, shifts),
        in_specs=[pl.BlockSpec(memory_space=pltpu.SMEM)]
        + [anywhere] * (1 + len(pieces) + len(out)),
        out_specs=anywhere,
        out_shape=jax.ShapeDtypeStruct((here, D), BF16),
        scratch_shapes=[
            pltpu.VMEM((n, here, M), BF16),
            pltpu.VMEM((n, here, DH), BF16),
            pltpu.VMEM((len(pieces), 4, M, DH), BF16),
            pltpu.SemaphoreType.DMA((n,)),
            pltpu.SemaphoreType.DMA((n,)),
            pltpu.SemaphoreType.DMA((len(pieces),)),
        ],
        input_output_aliases={2 + len(pieces): 0} if out else {},
    )(pos, weights, *pieces, *out)


def call(kernel, grid, in_specs, out_spec, out_shape, scratch, prefetch=1):
    return pl.pallas_call(
        kernel,
        grid_spec=pltpu.PrefetchScalarGridSpec(
            num_scalar_prefetch=prefetch,
            grid=grid,
            in_specs=in_specs,
            out_specs=out_spec,
            scratch_shapes=scratch,
        ),
        out_shape=out_shape,
        compiler_params=pltpu.CompilerParams(dimension_semantics=("arbitrary",) * len(grid)),
    )


def landmarks(tokens, per_device):
    segment = tokens.shape[0] // per_device
    sums = jnp.sum(tokens.reshape(per_device, segment, D), axis=1, dtype=F32)
    return (sums / segment).astype(BF16)


def steps(queries, keys, values):
    pos = jnp.stack([lax.axis_index(a) for a in SEQ]).astype(jnp.int32)
    here = queries.shape[0]
    per_device = M // 32
    q_a, q_b = gather_rows(landmarks(queries, per_device))
    k_a, k_b = gather_rows(landmarks(keys, per_device))

    column = pl.BlockSpec((here, GROUP * DH), lambda h, pos: (0, h))
    per_head = piece_specs(lambda h, pos: h, GROUP)
    land = pltpu.VMEM((M, GROUP * DH), BF16)
    table = pltpu.SMEM((64,), jnp.int32)
    parts = call(
        parts_kernel,
        (H // GROUP,),
        [column, column] + per_head,
        pl.BlockSpec((GROUP, M + EXTRA, DH), lambda h, pos: (h, 0, 0)),
        jax.ShapeDtypeStruct((H, M + EXTRA, DH), BF16),
        [land, table],
    )(pos, keys, values, *q_a, *q_b)
    parts = lax.all_to_all(parts, SEQ, split_axis=0, concat_axis=0, tiled=True)

    weights = call(
        near_kernel,
        (H // GROUP,),
        [column] + per_head,
        pl.BlockSpec((GROUP, here, M), lambda h, pos: (h, 0, 0)),
        jax.ShapeDtypeStruct((H, here, M), BF16),
        [land, table],
    )(pos, queries, *k_a, *k_b)

    owned = piece_specs(lambda g, pos: place(pos, 0, 0, 0), 1)
    inverse = call(
        inverse_kernel,
        (1,),
        owned + owned,
        pl.BlockSpec((M, M), lambda g, pos: (0, 0)),
        jax.ShapeDtypeStruct((M, M), BF16),
        [pltpu.VMEM((M, DH), BF16)] * 2 + [table],
    )(pos, *q_a, *q_b, *k_a, *k_b)

    product = call(
        product_kernel,
        (4,),
        [
            pl.BlockSpec((H, DH, 128), lambda c: (0, c, 0)),
            pl.BlockSpec((H, EXTRA, 128), lambda c: (0, M // EXTRA, 0)),
            pl.BlockSpec((M, 128), lambda c: (0, c)),
        ],
        pl.BlockSpec((M, DH), lambda c: (0, 0)),
        jax.ShapeDtypeStruct((M, DH), BF16),
        [pltpu.VMEM((M, DH), F32)],
        prefetch=0,
    )(parts, parts, inverse)

    other = shifted(product, "y", 1)
    lower = pos[2] == 0
    a = jnp.where(lower, product, other)
    b = jnp.where(lower, other, product)
    a = jnp.stack(in_slots(ring(a, "x")))
    b = jnp.stack(in_slots(ring(b, "z")))
    out = final((0,), pos, weights, [a, b])
    pieces = {}
    for s in (1, 3, 2):
        pieces[s] = [shifted(a, "z", s), shifted(b, "x", s)]
    out = final((1,), pos, weights, pieces[1], out)
    return final((3, 2), pos, weights, pieces[3] + pieces[2], out)


def solution(mesh):
    torus = Mesh(mesh.devices.reshape(4, 4, 2, mesh.shape["doc"]), ("x", "z", "y", "doc"))
    spec = P(DOC_SEQ, None)
    return jax.shard_map(
        steps, mesh=torus, in_specs=(spec, spec, spec), out_specs=spec, check_vma=False
    )
```

```python
import functools
import math

import jax
import jax.numpy as jnp
from jax import lax
from jax.experimental import pallas as pl
from jax.experimental.pallas import tpu as pltpu
from jax.sharding import Mesh
from jax.sharding import PartitionSpec as P


H = 32
DH = 128
M = 512
ITERS = 6
D = 4096
SEQ = ("x", "z", "y")
DOC_SEQ = ("doc", "x", "z", "y")
C2 = DH ** (-0.5) * math.log2(math.e)
F32 = jnp.float32
BF16 = jnp.bfloat16
EXTRA = 16
ROWS = M // 32
GROUP = 4
LAST = 8
TALL = 128


def shifted(v, axis, by):
    n = lax.axis_size(axis)
    return lax.ppermute(v, axis, [(i, (i + by) % n) for i in range(n)])


def near_ring(v, axis):
    return shifted(v, axis, 1), shifted(v, axis, 3)


def ring(v, axis):
    one, three = near_ring(v, axis)
    return [v, one, shifted(v, axis, 2), three]


def forward(one, three, axis):
    half = one.shape[0] // 2
    return shifted(one[:half], axis, 1), shifted(three[half:], axis, 3)


def relayed_ring(v, axis):
    one, three = near_ring(v, axis)
    return [v, one, *forward(one, three, axis), three]


def gather_rows(v, second):
    both = jnp.stack([v, shifted(v, "y", 1)])
    half = both.shape[-1] // 2
    a = jnp.stack(ring(both[..., :half], "x"))
    b = jnp.stack(ring(both[..., half:], "z"))
    return second(a, "z"), second(b, "x")


def blocks(pieces):
    at = 0
    for piece in pieces:
        yield at // 4, at % 4, piece
        at += piece.shape[0]


def place(pos, slot_x, slot_z, slot_y):
    jx = (pos[0] + 4 - slot_x) % 4
    jz = (pos[1] + 4 - slot_z) % 4
    jy = (pos[2] + slot_y) % 2
    return (jx * 4 + jz) * 2 + jy


def fill_table(pos, table):
    for later in range(4):
        for early in range(4):
            for slot_y in range(2):
                at = (later * 4 + early) * 2 + slot_y
                table[at] = place(pos, early, later, slot_y) * ROWS
                table[32 + at] = place(pos, later, early, slot_y) * ROWS


def spread(table, base, pieces, out):
    for later, first, piece in blocks(pieces):
        for early in range(piece.shape[0]):
            for slot_y in range(2):
                slot = (later * 4 + first + early) * 2 + slot_y
                at = pl.multiple_of(table[base + slot], ROWS)
                out[pl.ds(at, ROWS), :] = piece[early, slot_y]


def spread_head(table, head, pieces, out):
    half = len(pieces) // 2

    @pl.when(head < H // 2)
    def _():
        spread(table, 0, pieces[:half], out)

    @pl.when(head >= H // 2)
    def _():
        spread(table, 32, pieces[half:], out)


def piece_specs(pieces, block_of, heads):
    last = H // 2 // heads
    specs = []
    for i, piece in enumerate(pieces):
        shape = (piece.shape[0], 2, ROWS, heads * DH)
        if i < len(pieces) // 2:
            column = lambda *g: jnp.minimum(block_of(*g), last - 1)
        else:
            column = lambda *g: jnp.maximum(block_of(*g) - last, 0)
        specs.append(pl.BlockSpec(shape, lambda *g, column=column: (0, 0, 0, column(*g))))
    return specs


def nt(a, b):
    return lax.dot_general(a, b, (((1,), (1,)), ((), ())), preferred_element_type=F32)


def parts_kernel(pos, keys, values, *rest):
    pieces, (out, land, table) = rest[:-3], rest[-3:]
    g = pl.program_id(0)

    @pl.when(g == 0)
    def _():
        fill_table(pos, table)

    spread_head(table, g * GROUP, pieces, land)

    def scores_of(j):
        return nt(keys[:, j * DH : (j + 1) * DH], land[:, j * DH : (j + 1) * DH])

    def expo_of(scores):
        top = jnp.max(scores, 0, keepdims=True)
        expo = jnp.exp2(scores * C2 - top * C2)
        return top, expo.astype(BF16), jnp.sum(expo, 0, keepdims=True)

    def store(j, top, expo, totals):
        weighted = lax.dot_general(
            values[:, j * DH : (j + 1) * DH],
            expo,
            (((0,), (0,)), ((), ())),
            preferred_element_type=F32,
        )
        part = (weighted * (1.0 / totals)).astype(BF16)
        level = top * C2 + jnp.log2(totals)
        high = level.astype(BF16).astype(F32)
        mid = (level - high).astype(BF16).astype(F32)
        low = level - high - mid
        rows = []
        for k in range(0, M, 128):
            at = slice(k, k + 128)
            out[j, at, :] = part[:, at]
            rows += [high[:, at], mid[:, at], low[:, at]]
        rows.append(jnp.zeros((EXTRA - 12, 128), F32))
        out[j, M : M + EXTRA, :] = jnp.concatenate(rows, 0).astype(BF16)

    scores = scores_of(0)
    ready = None
    for j in range(GROUP):
        following = scores_of(j + 1) if j + 1 < GROUP else None
        current = expo_of(scores)
        if ready is not None:
            store(j - 1, *ready)
        ready, scores = current, following
    store(GROUP - 1, *ready)


def near_kernel(pos, queries, *rest):
    pieces, (out, land, table) = rest[:-3], rest[-3:]
    g = pl.program_id(0)

    @pl.when(g == 0)
    def _():
        fill_table(pos, table)

    spread_head(table, g * GROUP, pieces, land)
    for j in range(GROUP):
        cols = slice(j * DH, (j + 1) * DH)
        for t in range(0, queries.shape[0], TALL):
            near = nt(queries[t : t + TALL, cols], land[:, cols])
            top = jnp.max(near, 1, keepdims=True)
            expo = jnp.exp2(near * C2 - top * C2)
            totals = jnp.sum(expo, 1, keepdims=True)
            out[j, t : t + TALL] = (expo * (1.0 / totals)).astype(BF16)


def inverse_kernel(n_q, pos, *rest):
    pieces, (out, land_q, land_k, table) = rest[:-4], rest[-4:]
    fill_table(pos, table)
    head = place(pos, 0, 0, 0)
    spread_head(table, head, pieces[:n_q], land_q)
    spread_head(table, head, pieces[n_q:], land_k)
    scores = nt(land_q[...], land_k[...])
    top = jnp.max(scores, 1, keepdims=True)
    expo = jnp.exp2((scores - top) * C2)
    kernel = expo / jnp.sum(expo, 1, keepdims=True)
    row_most = jnp.max(jnp.sum(jnp.abs(kernel), 1, keepdims=True))
    col_most = jnp.max(jnp.sum(jnp.abs(kernel), 0, keepdims=True))
    low = kernel.astype(BF16)
    inverse = kernel.T / (row_most * col_most)

    def dot(a, b):
        return jnp.dot(a, b, preferred_element_type=F32)

    def sweep(_, inverse):
        inv = inverse.astype(BF16)
        prod = dot(low, inv)
        p = prod.astype(BF16)
        inner = 7.0 * prod - dot(p, p)
        middle = 15.0 * prod - dot(p, inner.astype(BF16))
        return 0.25 * (13.0 * inverse - dot(inv, middle.astype(BF16)))

    out[...] = lax.fori_loop(0, ITERS, sweep, inverse).astype(BF16)


def product_kernel(parts, levels, inverse, out, acc, shares):
    c = pl.program_id(0)

    @pl.when(c == 0)
    def _():
        for k in range(4):
            high, mid, low = (levels[:, 3 * k + t, :].astype(F32) for t in range(3))
            level = high + mid + low
            weight = jnp.exp2(level - jnp.max(level, 0, keepdims=True))
            shares[k] = weight / jnp.sum(weight, 0, keepdims=True)

    weight = shares[c]
    normed = jnp.zeros((128, 128), F32)
    for s in range(32):
        normed = normed + parts[s].astype(F32) * weight[s : s + 1]
    part = nt(inverse[...], normed.astype(BF16))

    @pl.when(c == 0)
    def _():
        acc[...] = part

    @pl.when(c > 0)
    def _():
        acc[...] += part

    @pl.when(c == 3)
    def _():
        out[...] = acc[...].astype(BF16)


def final_kernel(shifts, n_given, pos, weights, *rest):
    n = LAST * len(shifts)
    given = rest[:n_given]
    out, tiles, results, prods, sems_in, sems_out, sems_prod = rest[-7:]
    heads = []
    for shift in shifts:
        x, z = (pos[0] + 4 - shift) % 4, (pos[1] + 4 - shift) % 4
        heads += [(((pos[0] + 4 - early) % 4) * 4 + z) * 2 for early in range(4)]
        heads += [(x * 4 + (pos[1] + 4 - early) % 4) * 2 + 1 for early in range(4)]
    pieces = [
        pltpu.make_async_copy(
            piece, prods.at[later, pl.ds(early, piece.shape[0])], sems_prod.at[i]
        )
        for i, (later, early, piece) in enumerate(blocks(given))
    ]
    into = [
        pltpu.make_async_copy(weights.at[h], tiles.at[i], sems_in.at[i]) for i, h in enumerate(heads)
    ]
    back = [
        pltpu.make_async_copy(
            results.at[i],
            out.at[:, pl.ds(pl.multiple_of(h * DH, DH), DH)],
            sems_out.at[i],
        )
        for i, h in enumerate(heads)
    ]
    for copy in pieces + into:
        copy.start()
    for copy in pieces:
        copy.wait()
    for first in range(0, n, 4):
        for i in range(first, first + 4):
            into[i].wait()
        held = None
        for i in range(first, first + 4):
            both = jnp.dot(tiles[i], prods[i // 4, i % 4], preferred_element_type=F32)
            if held is not None:
                results[i - 1] = held.astype(BF16)
            held = both
        results[first + 3] = held.astype(BF16)
        for i in range(first, first + 4):
            back[i].start()
    for copy in back:
        copy.wait()


def final(shifts, pos, weights, pieces, *out):
    anywhere = pl.BlockSpec(memory_space=pl.ANY)
    here = weights.shape[1]
    n = LAST * len(shifts)
    return pl.pallas_call(
        functools.partial(final_kernel, shifts, len(pieces)),
        in_specs=[pl.BlockSpec(memory_space=pltpu.SMEM)]
        + [anywhere] * (1 + len(pieces) + len(out)),
        out_specs=anywhere,
        out_shape=jax.ShapeDtypeStruct((here, D), BF16),
        scratch_shapes=[
            pltpu.VMEM((n, here, M), BF16),
            pltpu.VMEM((n, here, DH), BF16),
            pltpu.VMEM((2 * len(shifts), 4, M, DH), BF16),
            pltpu.SemaphoreType.DMA((n,)),
            pltpu.SemaphoreType.DMA((n,)),
            pltpu.SemaphoreType.DMA((len(pieces),)),
        ],
        input_output_aliases={2 + len(pieces): 0} if out else {},
    )(pos, weights, *pieces, *out)


def call(kernel, grid, in_specs, out_spec, out_shape, scratch, prefetch=1):
    return pl.pallas_call(
        kernel,
        grid_spec=pltpu.PrefetchScalarGridSpec(
            num_scalar_prefetch=prefetch,
            grid=grid,
            in_specs=in_specs,
            out_specs=out_spec,
            scratch_shapes=scratch,
        ),
        out_shape=out_shape,
        compiler_params=pltpu.CompilerParams(dimension_semantics=("arbitrary",) * len(grid)),
    )


def landmarks(tokens, per_device):
    segment = tokens.shape[0] // per_device
    sums = jnp.sum(tokens.reshape(per_device, segment, D), axis=1, dtype=F32)
    return (sums / segment).astype(BF16)


def steps(queries, keys, values):
    pos = jnp.stack([lax.axis_index(a) for a in SEQ]).astype(jnp.int32)
    here = queries.shape[0]
    per_device = M // 32
    q_a, q_b = gather_rows(landmarks(queries, per_device), relayed_ring)
    k_a, k_b = gather_rows(landmarks(keys, per_device), ring)
    land_q, land_k = q_a + q_b, k_a + k_b

    column = pl.BlockSpec((here, GROUP * DH), lambda h, pos: (0, h))

    def per_head(pieces):
        return piece_specs(pieces, lambda h, pos: h, GROUP)

    land = pltpu.VMEM((M, GROUP * DH), BF16)
    table = pltpu.SMEM((64,), jnp.int32)
    parts = call(
        parts_kernel,
        (H // GROUP,),
        [column, column] + per_head(land_q),
        pl.BlockSpec((GROUP, M + EXTRA, DH), lambda h, pos: (h, 0, 0)),
        jax.ShapeDtypeStruct((H, M + EXTRA, DH), BF16),
        [land, table],
    )(pos, keys, values, *land_q)
    parts = lax.all_to_all(parts, SEQ, split_axis=0, concat_axis=0, tiled=True)

    weights = call(
        near_kernel,
        (H // GROUP,),
        [column] + per_head(land_k),
        pl.BlockSpec((GROUP, here, M), lambda h, pos: (h, 0, 0)),
        jax.ShapeDtypeStruct((H, here, M), BF16),
        [land, table],
    )(pos, queries, *land_k)


    def owned(pieces):
        return piece_specs(pieces, lambda g, pos: place(pos, 0, 0, 0), 1)

    inverse = call(
        functools.partial(inverse_kernel, len(land_q)),
        (1,),
        owned(land_q) + owned(land_k),
        pl.BlockSpec((M, M), lambda g, pos: (0, 0)),
        jax.ShapeDtypeStruct((M, M), BF16),
        [pltpu.VMEM((M, DH), BF16)] * 2 + [table],
    )(pos, *land_q, *land_k)

    product = call(
        product_kernel,
        (4,),
        [
            pl.BlockSpec((H, DH, 128), lambda c: (0, c, 0)),
            pl.BlockSpec((H, EXTRA, 128), lambda c: (0, M // EXTRA, 0)),
            pl.BlockSpec((M, 128), lambda c: (0, c)),
        ],
        pl.BlockSpec((M, DH), lambda c: (0, 0)),
        jax.ShapeDtypeStruct((M, DH), BF16),
        [pltpu.VMEM((M, DH), F32), pltpu.VMEM((4, 32, 128), F32)],
        prefetch=0,
    )(parts, parts, inverse)

    other = shifted(product, "y", 1)
    lower = pos[2] == 0
    a = jnp.where(lower, product, other)
    b = jnp.where(lower, other, product)
    a = jnp.stack(ring(a, "x"))
    b = jnp.stack(ring(b, "z"))
    out = final((0,), pos, weights, [a, b])
    a_one, a_three = near_ring(a, "z")
    b_one, b_three = near_ring(b, "x")
    far = [*forward(a_one, a_three, "z"), *forward(b_one, b_three, "x")]
    out = final((1, 3), pos, weights, [a_one, b_one, a_three, b_three], out)
    return final((2,), pos, weights, far, out)


def solution(mesh):
    torus = Mesh(mesh.devices.reshape(4, 4, 2, mesh.shape["doc"]), ("x", "z", "y", "doc"))
    spec = P(DOC_SEQ, None)
    return jax.shard_map(
        steps, mesh=torus, in_specs=(spec, spec, spec), out_specs=spec, check_vma=False
    )
```

```python
import functools
import math

import jax
import jax.numpy as jnp
from jax import lax
from jax.experimental import pallas as pl
from jax.experimental.pallas import tpu as pltpu
from jax.sharding import Mesh
from jax.sharding import PartitionSpec as P


H = 32
DH = 128
M = 512
ITERS = 6
D = 4096
SEQ = ("x", "z", "y")
DOC_SEQ = ("doc", "x", "z", "y")
C2 = DH ** (-0.5) * math.log2(math.e)
F32 = jnp.float32
BF16 = jnp.bfloat16
EXTRA = 16
ROWS = M // 32
GROUP = 4
LAST = 8
TALL = 128


def shifted(v, axis, by):
    n = lax.axis_size(axis)
    return lax.ppermute(v, axis, [(i, (i + by) % n) for i in range(n)])


def near_ring(v, axis):
    return shifted(v, axis, 1), shifted(v, axis, 3)


def ring(v, axis):
    one, three = near_ring(v, axis)
    return [v, one, shifted(v, axis, 2), three]


def forward(one, three, axis):
    half = one.shape[0] // 2
    return shifted(one[:half], axis, 1), shifted(three[half:], axis, 3)


def relayed_ring(v, axis):
    one, three = near_ring(v, axis)
    return [v, one, *forward(one, three, axis), three]


def gather_first(v):
    other = shifted(v, "y", 1)
    a = jnp.stack(ring(v, "x"))
    b = jnp.stack(ring(other, "z"))
    return a, b


def gather_rows(v, second):
    a, b = gather_first(v)
    return second(a, "z") + second(b, "x")


def blocks(pieces):
    at = 0
    for piece in pieces:
        yield at // 4, at % 4, piece
        at += piece.shape[0]


def place(pos, slot_x, slot_z, slot_y):
    jx = (pos[0] + 4 - slot_x) % 4
    jz = (pos[1] + 4 - slot_z) % 4
    jy = (pos[2] + slot_y) % 2
    return (jx * 4 + jz) * 2 + jy


def fill_table(pos, table):
    for later in range(4):
        for early in range(4):
            table[later * 4 + early] = place(pos, early, later, 0) * ROWS
            table[16 + later * 4 + early] = place(pos, later, early, 1) * ROWS


def spread(table, pieces, out):
    half = len(pieces) // 2
    for base, some in ((0, pieces[:half]), (16, pieces[half:])):
        for later, first, piece in blocks(some):
            for early in range(piece.shape[0]):
                at = pl.multiple_of(table[base + later * 4 + first + early], ROWS)
                out[pl.ds(at, ROWS), :] = piece[early]


def piece_specs(pieces, block_of, heads):
    return [
        pl.BlockSpec((piece.shape[0], ROWS, heads * DH), lambda *g: (0, 0, block_of(*g)))
        for piece in pieces
    ]


def nt(a, b):
    return lax.dot_general(a, b, (((1,), (1,)), ((), ())), preferred_element_type=F32)


def parts_kernel(pos, keys, values, *rest):
    pieces, (out, land, table) = rest[:-3], rest[-3:]
    g = pl.program_id(0)

    @pl.when(g == 0)
    def _():
        fill_table(pos, table)

    spread(table, pieces, land)

    def scores_of(j):
        return nt(keys[:, j * DH : (j + 1) * DH], land[:, j * DH : (j + 1) * DH])

    def expo_of(scores):
        top = jnp.max(scores, 0, keepdims=True)
        expo = jnp.exp2(scores * C2 - top * C2)
        return top, expo.astype(BF16), jnp.sum(expo, 0, keepdims=True)

    def store(j, top, expo, totals):
        weighted = lax.dot_general(
            values[:, j * DH : (j + 1) * DH],
            expo,
            (((0,), (0,)), ((), ())),
            preferred_element_type=F32,
        )
        part = (weighted * (1.0 / totals)).astype(BF16)
        level = top * C2 + jnp.log2(totals)
        high = level.astype(BF16).astype(F32)
        mid = (level - high).astype(BF16).astype(F32)
        low = level - high - mid
        rows = []
        for k in range(0, M, 128):
            at = slice(k, k + 128)
            out[j, at, :] = part[:, at]
            rows += [high[:, at], mid[:, at], low[:, at]]
        rows.append(jnp.zeros((EXTRA - 12, 128), F32))
        out[j, M : M + EXTRA, :] = jnp.concatenate(rows, 0).astype(BF16)

    scores = scores_of(0)
    ready = None
    for j in range(GROUP):
        following = scores_of(j + 1) if j + 1 < GROUP else None
        current = expo_of(scores)
        if ready is not None:
            store(j - 1, *ready)
        ready, scores = current, following
    store(GROUP - 1, *ready)


def near_kernel(pos, queries, *rest):
    pieces, (out, land, table) = rest[:-3], rest[-3:]
    g = pl.program_id(0)

    @pl.when(g == 0)
    def _():
        fill_table(pos, table)

    spread(table, pieces, land)
    for j in range(GROUP):
        cols = slice(j * DH, (j + 1) * DH)
        for t in range(0, queries.shape[0], TALL):
            near = nt(queries[t : t + TALL, cols], land[:, cols])
            top = jnp.max(near, 1, keepdims=True)
            expo = jnp.exp2(near * C2 - top * C2)
            totals = jnp.sum(expo, 1, keepdims=True)
            out[j, t : t + TALL] = (expo * (1.0 / totals)).astype(BF16)


def inverse_kernel(n_q, pos, *rest):
    pieces, (out, land_q, land_k, table) = rest[:-4], rest[-4:]
    fill_table(pos, table)
    spread(table, pieces[:n_q], land_q)
    spread(table, pieces[n_q:], land_k)
    scores = nt(land_q[...], land_k[...])
    top = jnp.max(scores, 1, keepdims=True)
    expo = jnp.exp2((scores - top) * C2)
    kernel = expo / jnp.sum(expo, 1, keepdims=True)
    row_most = jnp.max(jnp.sum(jnp.abs(kernel), 1, keepdims=True))
    col_most = jnp.max(jnp.sum(jnp.abs(kernel), 0, keepdims=True))
    low = kernel.astype(BF16)
    inverse = kernel.T / (row_most * col_most)

    def dot(a, b):
        return jnp.dot(a, b, preferred_element_type=F32)

    def sweep(_, inverse):
        inv = inverse.astype(BF16)
        prod = dot(low, inv)
        p = prod.astype(BF16)
        inner = 7.0 * prod - dot(p, p)
        middle = 15.0 * prod - dot(p, inner.astype(BF16))
        return 0.25 * (13.0 * inverse - dot(inv, middle.astype(BF16)))

    out[...] = lax.fori_loop(0, ITERS, sweep, inverse).astype(BF16)


def product_kernel(parts, levels, inverse, out, acc, shares):
    c = pl.program_id(0)

    @pl.when(c == 0)
    def _():
        for k in range(4):
            high, mid, low = (levels[:, 3 * k + t, :].astype(F32) for t in range(3))
            level = high + mid + low
            weight = jnp.exp2(level - jnp.max(level, 0, keepdims=True))
            shares[k] = weight / jnp.sum(weight, 0, keepdims=True)

    weight = shares[c]
    normed = jnp.zeros((128, 128), F32)
    for s in range(32):
        normed = normed + parts[s].astype(F32) * weight[s : s + 1]
    part = nt(inverse[...], normed.astype(BF16))

    @pl.when(c == 0)
    def _():
        acc[...] = part

    @pl.when(c > 0)
    def _():
        acc[...] += part

    @pl.when(c == 3)
    def _():
        out[...] = acc[...].astype(BF16)


def final_kernel(shifts, n_given, pos, weights, *rest):
    n = LAST * len(shifts)
    given = rest[:n_given]
    out, tiles, results, prods, sems_in, sems_out, sems_prod = rest[-7:]
    heads = []
    for shift in shifts:
        x, z = (pos[0] + 4 - shift) % 4, (pos[1] + 4 - shift) % 4
        y = pos[2]
        heads += [(((pos[0] + 4 - early) % 4) * 4 + z) * 2 + y for early in range(4)]
        heads += [(x * 4 + (pos[1] + 4 - early) % 4) * 2 + 1 - y for early in range(4)]
    pieces = [
        pltpu.make_async_copy(
            piece, prods.at[later, pl.ds(early, piece.shape[0])], sems_prod.at[i]
        )
        for i, (later, early, piece) in enumerate(blocks(given))
    ]
    into = [
        pltpu.make_async_copy(weights.at[h], tiles.at[i], sems_in.at[i]) for i, h in enumerate(heads)
    ]
    back = [
        pltpu.make_async_copy(
            results.at[i],
            out.at[:, pl.ds(pl.multiple_of(h * DH, DH), DH)],
            sems_out.at[i],
        )
        for i, h in enumerate(heads)
    ]
    for copy in pieces + into:
        copy.start()
    for copy in pieces:
        copy.wait()
    for first in range(0, n, 4):
        for i in range(first, first + 4):
            into[i].wait()
        held = None
        for i in range(first, first + 4):
            both = jnp.dot(tiles[i], prods[i // 4, i % 4], preferred_element_type=F32)
            if held is not None:
                results[i - 1] = held.astype(BF16)
            held = both
        results[first + 3] = held.astype(BF16)
        for i in range(first, first + 4):
            back[i].start()
    for copy in back:
        copy.wait()


def final(shifts, pos, weights, pieces, *out):
    anywhere = pl.BlockSpec(memory_space=pltpu.HBM)
    here = weights.shape[1]
    n = LAST * len(shifts)
    return pl.pallas_call(
        functools.partial(final_kernel, shifts, len(pieces)),
        in_specs=[pl.BlockSpec(memory_space=pltpu.SMEM)]
        + [anywhere] * (1 + len(pieces) + len(out)),
        out_specs=anywhere,
        out_shape=jax.ShapeDtypeStruct((here, D), BF16),
        scratch_shapes=[
            pltpu.VMEM((n, here, M), BF16),
            pltpu.VMEM((n, here, DH), BF16),
            pltpu.VMEM((2 * len(shifts), 4, M, DH), BF16),
            pltpu.SemaphoreType.DMA((n,)),
            pltpu.SemaphoreType.DMA((n,)),
            pltpu.SemaphoreType.DMA((len(pieces),)),
        ],
        input_output_aliases={2 + len(pieces): 0} if out else {},
    )(pos, weights, *pieces, *out)


def call(kernel, grid, in_specs, out_spec, out_shape, scratch, prefetch=1):
    return pl.pallas_call(
        kernel,
        grid_spec=pltpu.PrefetchScalarGridSpec(
            num_scalar_prefetch=prefetch,
            grid=grid,
            in_specs=in_specs,
            out_specs=out_spec,
            scratch_shapes=scratch,
        ),
        out_shape=out_shape,
        compiler_params=pltpu.CompilerParams(dimension_semantics=("arbitrary",) * len(grid)),
    )


def landmarks(tokens, per_device):
    segment = tokens.shape[0] // per_device
    sums = jnp.sum(tokens.reshape(per_device, segment, D), axis=1, dtype=F32)
    return (sums / segment).astype(BF16)


def steps(queries, keys, values):
    pos = jnp.stack([lax.axis_index(a) for a in SEQ]).astype(jnp.int32)
    here = queries.shape[0]
    per_device = M // 32
    land_q = gather_rows(landmarks(queries, per_device), relayed_ring)
    land_k = gather_rows(landmarks(keys, per_device), ring)

    column = pl.BlockSpec((here, GROUP * DH), lambda h, pos: (0, h))

    def per_head(pieces):
        return piece_specs(pieces, lambda h, pos: h, GROUP)

    land = pltpu.VMEM((M, GROUP * DH), BF16)
    table = pltpu.SMEM((32,), jnp.int32)
    parts = call(
        parts_kernel,
        (H // GROUP,),
        [column, column] + per_head(land_q),
        pl.BlockSpec((GROUP, M + EXTRA, DH), lambda h, pos: (h, 0, 0)),
        jax.ShapeDtypeStruct((H, M + EXTRA, DH), BF16),
        [land, table],
    )(pos, keys, values, *land_q)
    parts = lax.all_to_all(parts, SEQ, split_axis=0, concat_axis=0, tiled=True)

    weights = call(
        near_kernel,
        (H // GROUP,),
        [column] + per_head(land_k),
        pl.BlockSpec((GROUP, here, M), lambda h, pos: (h, 0, 0)),
        jax.ShapeDtypeStruct((H, here, M), BF16),
        [land, table],
    )(pos, queries, *land_k)


    def owned(pieces):
        return piece_specs(pieces, lambda g, pos: place(pos, 0, 0, 0), 1)

    inverse = call(
        functools.partial(inverse_kernel, len(land_q)),
        (1,),
        owned(land_q) + owned(land_k),
        pl.BlockSpec((M, M), lambda g, pos: (0, 0)),
        jax.ShapeDtypeStruct((M, M), BF16),
        [pltpu.VMEM((M, DH), BF16)] * 2 + [table],
    )(pos, *land_q, *land_k)

    product = call(
        product_kernel,
        (4,),
        [
            pl.BlockSpec((H, DH, 128), lambda c: (0, c, 0)),
            pl.BlockSpec((H, EXTRA, 128), lambda c: (0, M // EXTRA, 0)),
            pl.BlockSpec((M, 128), lambda c: (0, c)),
        ],
        pl.BlockSpec((M, DH), lambda c: (0, 0)),
        jax.ShapeDtypeStruct((M, DH), BF16),
        [pltpu.VMEM((M, DH), F32), pltpu.VMEM((4, 32, 128), F32)],
        prefetch=0,
    )(parts, parts, inverse)

    a, b = gather_first(product)
    out = final((0,), pos, weights, [a, b])
    a_one, a_three = near_ring(a, "z")
    b_one, b_three = near_ring(b, "x")
    far = [*forward(a_one, a_three, "z"), *forward(b_one, b_three, "x")]
    out = final((1, 3), pos, weights, [a_one, b_one, a_three, b_three], out)
    return final((2,), pos, weights, far, out)


def solution(mesh):
    torus = Mesh(mesh.devices.reshape(4, 4, 2, mesh.shape["doc"]), ("x", "z", "y", "doc"))
    spec = P(DOC_SEQ, None)
    return jax.shard_map(
        steps, mesh=torus, in_specs=(spec, spec, spec), out_specs=spec, check_vma=False
    )
```

```python
import functools
import math

import jax
import jax.numpy as jnp
from jax import lax
from jax.experimental import pallas as pl
from jax.experimental.pallas import tpu as pltpu
from jax.sharding import Mesh
from jax.sharding import PartitionSpec as P


H = 32
DH = 128
M = 512
ITERS = 6
D = 4096
SEQ = ("x", "z", "y")
DOC_SEQ = ("doc", "x", "z", "y")
C2 = DH ** (-0.5) * math.log2(math.e)
F32 = jnp.float32
BF16 = jnp.bfloat16
EXTRA = 16
ROWS = M // 32
GROUP = 4
LAST = 8
TALL = 128


def shifted(v, axis, by):
    n = lax.axis_size(axis)
    return lax.ppermute(v, axis, [(i, (i + by) % n) for i in range(n)])


def near_ring(v, axis):
    return shifted(v, axis, 1), shifted(v, axis, 3)


def ring(v, axis):
    one, three = near_ring(v, axis)
    return [v, one, shifted(v, axis, 2), three]


def forward(one, three, axis):
    half = one.shape[0] // 2
    return shifted(one[:half], axis, 1), shifted(three[half:], axis, 3)


def relayed_ring(v, axis):
    one, three = near_ring(v, axis)
    return [v, one, *forward(one, three, axis), three]


def gather_first(v):
    other = shifted(v, "y", 1)
    a = jnp.stack(ring(v, "x"))
    b = jnp.stack(ring(other, "z"))
    return a, b


def gather_rows(v, second):
    a, b = gather_first(v)
    return second(a, "z") + second(b, "x")


def blocks(pieces):
    at = 0
    for piece in pieces:
        yield at // 4, at % 4, piece
        at += piece.shape[0]


def place(pos, slot_x, slot_z, slot_y):
    jx = (pos[0] + 4 - slot_x) % 4
    jz = (pos[1] + 4 - slot_z) % 4
    jy = (pos[2] + slot_y) % 2
    return (jx * 4 + jz) * 2 + jy


def fill_table(pos, table):
    for later in range(4):
        for early in range(4):
            table[later * 4 + early] = place(pos, early, later, 0) * ROWS
            table[16 + later * 4 + early] = place(pos, later, early, 1) * ROWS


def spread(table, pieces, out):
    half = len(pieces) // 2
    for base, some in ((0, pieces[:half]), (16, pieces[half:])):
        for later, first, piece in blocks(some):
            for early in range(piece.shape[0]):
                at = pl.multiple_of(table[base + later * 4 + first + early], ROWS)
                out[pl.ds(at, ROWS), :] = piece[early]


def piece_specs(pieces, block_of, heads):
    return [
        pl.BlockSpec((piece.shape[0], ROWS, heads * DH), lambda *g: (0, 0, block_of(*g)))
        for piece in pieces
    ]


def nt(a, b):
    return lax.dot_general(a, b, (((1,), (1,)), ((), ())), preferred_element_type=F32)


def parts_kernel(pos, keys, values, *rest):
    pieces, (out, land, table) = rest[:-3], rest[-3:]
    g = pl.program_id(0)

    @pl.when(g == 0)
    def _():
        fill_table(pos, table)

    spread(table, pieces, land)

    def scores_of(j):
        return nt(keys[:, j * DH : (j + 1) * DH], land[:, j * DH : (j + 1) * DH])

    def expo_of(scores):
        top = jnp.max(scores, 0, keepdims=True)
        expo = jnp.exp2(scores * C2 - top * C2)
        return top, expo.astype(BF16), jnp.sum(expo, 0, keepdims=True)

    def store(j, top, expo, totals):
        weighted = lax.dot_general(
            values[:, j * DH : (j + 1) * DH],
            expo,
            (((0,), (0,)), ((), ())),
            preferred_element_type=F32,
        )
        part = (weighted * (1.0 / totals)).astype(BF16)
        level = top * C2 + jnp.log2(totals)
        high = level.astype(BF16).astype(F32)
        mid = (level - high).astype(BF16).astype(F32)
        low = level - high - mid
        rows = []
        for k in range(0, M, 128):
            at = slice(k, k + 128)
            out[j, at, :] = part[:, at]
            rows += [high[:, at], mid[:, at], low[:, at]]
        rows.append(jnp.zeros((EXTRA - 12, 128), F32))
        out[j, M : M + EXTRA, :] = jnp.concatenate(rows, 0).astype(BF16)

    scores = scores_of(0)
    ready = None
    for j in range(GROUP):
        following = scores_of(j + 1) if j + 1 < GROUP else None
        current = expo_of(scores)
        if ready is not None:
            store(j - 1, *ready)
        ready, scores = current, following
    store(GROUP - 1, *ready)


def near_kernel(pos, queries, *rest):
    pieces, (out, land, table) = rest[:-3], rest[-3:]
    g = pl.program_id(0)

    @pl.when(g == 0)
    def _():
        fill_table(pos, table)

    spread(table, pieces, land)
    for j in range(GROUP):
        cols = slice(j * DH, (j + 1) * DH)
        for t in range(0, queries.shape[0], TALL):
            near = nt(queries[t : t + TALL, cols], land[:, cols])
            top = jnp.max(near, 1, keepdims=True)
            expo = jnp.exp2(near * C2 - top * C2)
            totals = jnp.sum(expo, 1, keepdims=True)
            out[j, t : t + TALL] = (expo * (1.0 / totals)).astype(BF16)


def inverse_kernel(n_q, pos, *rest):
    pieces, (out, land_q, land_k, table) = rest[:-4], rest[-4:]
    fill_table(pos, table)
    spread(table, pieces[:n_q], land_q)
    spread(table, pieces[n_q:], land_k)
    scores = nt(land_q[...], land_k[...])
    top = jnp.max(scores, 1, keepdims=True)
    expo = jnp.exp2((scores - top) * C2)
    kernel = expo / jnp.sum(expo, 1, keepdims=True)
    row_most = jnp.max(jnp.sum(jnp.abs(kernel), 1, keepdims=True))
    col_most = jnp.max(jnp.sum(jnp.abs(kernel), 0, keepdims=True))
    low = kernel.astype(BF16)
    inverse = kernel.T / (row_most * col_most)

    def dot(a, b):
        return jnp.dot(a, b, preferred_element_type=F32)

    def sweep(_, inverse):
        inv = inverse.astype(BF16)
        prod = dot(low, inv)
        p = prod.astype(BF16)
        inner = 7.0 * prod - dot(p, p)
        middle = 15.0 * prod - dot(p, inner.astype(BF16))
        return 0.25 * (13.0 * inverse - dot(inv, middle.astype(BF16)))

    out[...] = lax.fori_loop(0, ITERS, sweep, inverse).astype(BF16)


def product_kernel(parts, levels, inverse, out, acc, shares):
    c = pl.program_id(0)

    @pl.when(c == 0)
    def _():
        for k in range(4):
            high, mid, low = (levels[:, 3 * k + t, :].astype(F32) for t in range(3))
            level = high + mid + low
            weight = jnp.exp2(level - jnp.max(level, 0, keepdims=True))
            shares[k] = weight / jnp.sum(weight, 0, keepdims=True)

    weight = shares[c]
    normed = jnp.zeros((128, 128), F32)
    for s in range(32):
        normed = normed + parts[s].astype(F32) * weight[s : s + 1]
    part = nt(inverse[...], normed.astype(BF16))

    @pl.when(c == 0)
    def _():
        acc[...] = part

    @pl.when(c > 0)
    def _():
        acc[...] += part

    @pl.when(c == 3)
    def _():
        out[...] = acc[...].astype(BF16)


def final_kernel(shifts, n_given, pos, weights, *rest):
    n = LAST * len(shifts)
    given = rest[:n_given]
    out, tiles, results, sems_in, sems_out = rest[-5:]
    heads = []
    for shift in shifts:
        x, z = (pos[0] + 4 - shift) % 4, (pos[1] + 4 - shift) % 4
        y = pos[2]
        heads += [(((pos[0] + 4 - early) % 4) * 4 + z) * 2 + y for early in range(4)]
        heads += [(x * 4 + (pos[1] + 4 - early) % 4) * 2 + 1 - y for early in range(4)]
    prods = [piece.at[e] for piece in given for e in range(piece.shape[0])]
    into = [
        pltpu.make_async_copy(weights.at[h], tiles.at[i], sems_in.at[i]) for i, h in enumerate(heads)
    ]
    back = [
        pltpu.make_async_copy(
            results.at[i],
            out.at[:, pl.ds(pl.multiple_of(h * DH, DH), DH)],
            sems_out.at[i],
        )
        for i, h in enumerate(heads)
    ]
    for copy in into:
        copy.start()
    for first in range(0, n, 4):
        for i in range(first, first + 4):
            into[i].wait()
        held = None
        for i in range(first, first + 4):
            both = jnp.dot(tiles[i], prods[i][...], preferred_element_type=F32)
            if held is not None:
                results[i - 1] = held.astype(BF16)
            held = both
        results[first + 3] = held.astype(BF16)
        for i in range(first, first + 4):
            back[i].start()
    for copy in back:
        copy.wait()


def final(shifts, pos, weights, pieces, *out):
    anywhere = pl.BlockSpec(memory_space=pltpu.HBM)
    here = weights.shape[1]
    n = LAST * len(shifts)
    return pl.pallas_call(
        functools.partial(final_kernel, shifts, len(pieces)),
        in_specs=[pl.BlockSpec(memory_space=pltpu.SMEM), anywhere]
        + [pl.BlockSpec(memory_space=pltpu.VMEM)] * len(pieces)
        + [anywhere] * len(out),
        out_specs=anywhere,
        out_shape=jax.ShapeDtypeStruct((here, D), BF16),
        scratch_shapes=[
            pltpu.VMEM((n, here, M), BF16),
            pltpu.VMEM((n, here, DH), BF16),
            pltpu.SemaphoreType.DMA((n,)),
            pltpu.SemaphoreType.DMA((n,)),
        ],
        input_output_aliases={2 + len(pieces): 0} if out else {},
        compiler_params=pltpu.CompilerParams(vmem_limit_bytes=24 << 20),
    )(pos, weights, *pieces, *out)


def call(kernel, grid, in_specs, out_spec, out_shape, scratch, prefetch=1):
    return pl.pallas_call(
        kernel,
        grid_spec=pltpu.PrefetchScalarGridSpec(
            num_scalar_prefetch=prefetch,
            grid=grid,
            in_specs=in_specs,
            out_specs=out_spec,
            scratch_shapes=scratch,
        ),
        out_shape=out_shape,
        compiler_params=pltpu.CompilerParams(dimension_semantics=("arbitrary",) * len(grid)),
    )


def landmarks(tokens, per_device):
    segment = tokens.shape[0] // per_device
    sums = jnp.sum(tokens.reshape(per_device, segment, D), axis=1, dtype=F32)
    return (sums / segment).astype(BF16)


def steps(queries, keys, values):
    pos = jnp.stack([lax.axis_index(a) for a in SEQ]).astype(jnp.int32)
    here = queries.shape[0]
    per_device = M // 32
    land_q = gather_rows(landmarks(queries, per_device), relayed_ring)
    land_k = gather_rows(landmarks(keys, per_device), ring)

    column = pl.BlockSpec((here, GROUP * DH), lambda h, pos: (0, h))

    def per_head(pieces):
        return piece_specs(pieces, lambda h, pos: h, GROUP)

    land = pltpu.VMEM((M, GROUP * DH), BF16)
    table = pltpu.SMEM((32,), jnp.int32)
    parts = call(
        parts_kernel,
        (H // GROUP,),
        [column, column] + per_head(land_q),
        pl.BlockSpec((GROUP, M + EXTRA, DH), lambda h, pos: (h, 0, 0)),
        jax.ShapeDtypeStruct((H, M + EXTRA, DH), BF16),
        [land, table],
    )(pos, keys, values, *land_q)
    parts = lax.all_to_all(parts, SEQ, split_axis=0, concat_axis=0, tiled=True)

    weights = call(
        near_kernel,
        (H // GROUP,),
        [column] + per_head(land_k),
        pl.BlockSpec((GROUP, here, M), lambda h, pos: (h, 0, 0)),
        jax.ShapeDtypeStruct((H, here, M), BF16),
        [land, table],
    )(pos, queries, *land_k)


    def owned(pieces):
        return piece_specs(pieces, lambda g, pos: place(pos, 0, 0, 0), 1)

    inverse = call(
        functools.partial(inverse_kernel, len(land_q)),
        (1,),
        owned(land_q) + owned(land_k),
        pl.BlockSpec((M, M), lambda g, pos: (0, 0)),
        jax.ShapeDtypeStruct((M, M), BF16),
        [pltpu.VMEM((M, DH), BF16)] * 2 + [table],
    )(pos, *land_q, *land_k)

    product = call(
        product_kernel,
        (4,),
        [
            pl.BlockSpec((H, DH, 128), lambda c: (0, c, 0)),
            pl.BlockSpec((H, EXTRA, 128), lambda c: (0, M // EXTRA, 0)),
            pl.BlockSpec((M, 128), lambda c: (0, c)),
        ],
        pl.BlockSpec((M, DH), lambda c: (0, 0)),
        jax.ShapeDtypeStruct((M, DH), BF16),
        [pltpu.VMEM((M, DH), F32), pltpu.VMEM((4, 32, 128), F32)],
        prefetch=0,
    )(parts, parts, inverse)

    a, b = gather_first(product)
    out = final((0,), pos, weights, [a, b])
    a_one, a_three = near_ring(a, "z")
    b_one, b_three = near_ring(b, "x")
    far = [*forward(a_one, a_three, "z"), *forward(b_one, b_three, "x")]
    out = final((1, 3), pos, weights, [a_one, b_one, a_three, b_three], out)
    return final((2,), pos, weights, far, out)


def solution(mesh):
    torus = Mesh(mesh.devices.reshape(4, 4, 2, mesh.shape["doc"]), ("x", "z", "y", "doc"))
    spec = P(DOC_SEQ, None)
    return jax.shard_map(
        steps, mesh=torus, in_specs=(spec, spec, spec), out_specs=spec, check_vma=False
    )
```
